32 devices in a mesh: dp: 2 (over x), row: 4 (over y, core), col: 4 (over z).
Axes of the slice: x: 2, y: 2, z: 4, core: 2. Of those that a mesh axis runs over, the one named last changes fastest.
Arguments:
- latents: float32 [24, 32, 128], P(('dp', 'row')), may hold values from -6 to 6
- labels: int32 [24], P(('dp', 'row')), may hold values from 0 to 999
- step_index: int32 [24], P(('dp', 'row')), may hold values from 1 to 8
- seeds: int32 [24], P(('dp', 'row')), may hold values from 0 to 2147483646
- class_table: bfloat16 [1000, 1152], replicated, may hold values from -6 to 6
- teacher_patch: bfloat16 [16, 1152], replicated, may hold values from -1.5 to 1.5
- teacher_mod: bfloat16 [1152, 3, 1152], P(('dp', 'row'), None, 'col'), may hold values from -0.1875 to 0.1875
- teacher_up: bfloat16 [1152, 4608], P(('dp', 'row'), 'col'), may hold values from -0.1875 to 0.1875
- teacher_down: bfloat16 [1152, 4608], P(('dp', 'row'), 'col'), may hold values from -0.09375 to 0.09375
- teacher_out: bfloat16 [16, 1152], replicated, may hold values from -0.1875 to 0.1875
- student_patch: bfloat16 [16, 1152], replicated, may hold values from -1.5 to 1.5
- student_mod: bfloat16 [1152, 3, 1152], P(('dp', 'row'), None, 'col'), may hold values from -0.1875 to 0.1875
- student_up: bfloat16 [1152, 4608], P(('dp', 'row'), 'col'), may hold values from -0.1875 to 0.1875
- student_down: bfloat16 [1152, 4608], P(('dp', 'row'), 'col'), may hold values from -0.09375 to 0.09375
- student_out: bfloat16 [16, 1152], replicated, may hold values from -0.1875 to 0.1875
Outputs:
- up_gradient: float32 [1152, 4608], P(('dp', 'row'), 'col')
- down_gradient: float32 [1152, 4608], P(('dp', 'row'), 'col')
The draws below stay inside these ranges and needn't reach their ends.
All inputs are finite; a program needn't handle non-finite values.
Results may differ from the reference program's by a relative error of at most 0.002.
Values may be sent and summed in bfloat16 or wider, within the bound.
A program may use at most 128 MiB of HBM per device.

```python
import math
import jax
import jax.numpy as jnp
from jax import lax

D = 1152
FF = 4608
CLASSES = 1000
SEQ = 256
PATCH = 16
STEPS = 8
BATCH = 24
N_COL = 4


def touch_ends(values, own_key, smallest, high):
    shape = values.shape
    spot = [jax.random.randint(jax.random.fold_in(own_key, axis), (), 0, shape[axis]) for axis in range(len(shape))]
    values = values.at[tuple(spot)].set(smallest)
    longest = shape.index(max(shape))
    spot[longest] = (spot[longest] + 1) % shape[longest]
    return values.at[tuple(spot)].set(high)


def levels(own_key, shape, shards, least, high):
    gain, own = 1.0, jax.random.fold_in(own_key, 6)
    for dim, shards_of in shards:
        draws = jnp.exp(jax.random.uniform(jax.random.fold_in(own, dim), (shards_of,), jnp.float32, least / len(shards), high / len(shards)))
        gain = gain * jnp.repeat(draws, shape[dim] // shards_of).reshape([-1 if axis == dim else 1 for axis in range(len(shape))])
    return gain


def gaussian(stream_key, shape, deviation, reach, split=(), held_as=jnp.bfloat16):
    entries = deviation * jax.random.normal(stream_key, shape, jnp.float32)
    if split:
        entries = entries * levels(stream_key, shape, split, -0.22, 0.18)
    return jnp.clip(entries, -reach, reach).astype(held_as)


def setup_inputs(seed: int = 0) -> dict:
    streams_of = jax.random.split(jax.random.key(seed), 16)
    return {
        "latents": gaussian(streams_of[0], (BATCH, SEQ * PATCH // 128, 128), 1.0, 6.0, ((0, 8),), jnp.float32),
        "labels": touch_ends(jax.random.randint(streams_of[1], (BATCH,), 0, CLASSES), jax.random.fold_in(streams_of[1], 1), 0, CLASSES - 1).astype(jnp.int32),
        "step_index": touch_ends(jax.random.randint(streams_of[2], (BATCH,), 1, STEPS + 1), jax.random.fold_in(streams_of[2], 1), 1, STEPS).astype(jnp.int32),
        "seeds": touch_ends(jax.random.randint(streams_of[3], (BATCH,), 0, 2147483647), jax.random.fold_in(streams_of[3], 1), 0, 2147483646).astype(jnp.int32),
        "class_table": gaussian(streams_of[4], (CLASSES, D), 1.0, 6.0),
        "teacher_patch": gaussian(streams_of[5], (PATCH, D), PATCH ** -0.5, 1.5),
        "teacher_mod": gaussian(streams_of[6], (D, 3, D), D ** -0.5, 0.1875, ((0, 8), (2, 4))),
        "teacher_up": gaussian(streams_of[7], (D, FF), D ** -0.5, 0.1875, ((0, 8), (1, 4))),
        "teacher_down": gaussian(streams_of[8], (D, FF), FF ** -0.5, 0.09375, ((0, 8), (1, 4))),
        "teacher_out": gaussian(streams_of[9], (PATCH, D), D ** -0.5, 0.1875),
        "student_patch": gaussian(streams_of[10], (PATCH, D), PATCH ** -0.5, 1.5),
        "student_mod": gaussian(streams_of[11], (D, 3, D), D ** -0.5, 0.1875, ((0, 8), (2, 4))),
        "student_up": gaussian(streams_of[12], (D, FF), D ** -0.5, 0.1875, ((0, 8), (1, 4))),
        "student_down": gaussian(streams_of[13], (D, FF), FF ** -0.5, 0.09375, ((0, 8), (1, 4))),
        "student_out": gaussian(streams_of[14], (PATCH, D), D ** -0.5, 0.1875),
    }


HALF_PI = 0.5 * math.pi
ROOT_TWO_PI = math.sqrt(2.0 / math.pi)

def plan(times):
    return (jnp.cos(HALF_PI * times), jnp.sin(HALF_PI * times))

def mixing(value):
    amount = jnp.int32(16)
    value = value ^ lax.shift_right_logical(value, amount)
    value = value * 73244475
    value = value ^ lax.shift_right_logical(value, amount)
    value = value * 73244475
    value = value ^ lax.shift_right_logical(value, amount)
    return value

def noise_of(seeds):
    total = SEQ * PATCH
    places = jnp.arange(total, dtype=jnp.int32).reshape(1, total // 128, 128)
    mixed = mixing(seeds[:, None, None] * 1103515245 + places * 40503 + 12345)
    uniform = (lax.shift_right_logical(mixed, jnp.int32(8)).astype(jnp.float32) + 0.5) * (1.0 / 16777216.0)
    return math.sqrt(2.0) * lax.erf_inv(2.0 * uniform - 1.0)

def time_features(times):
    half = D // 2
    freqs = jnp.exp(-math.log(10000.0) * jnp.arange(half, dtype=jnp.float32) / half)
    angle = (1000.0 * times)[:, None] * freqs[None, :]
    return jnp.concatenate([jnp.cos(angle), jnp.sin(angle)], axis=1)

def condition(times, labels, class_table):
    onehot = (labels[:, None] == jnp.arange(CLASSES, dtype=jnp.int32)[None, :]).astype(jnp.bfloat16)
    embedded = jnp.dot(onehot, class_table, preferred_element_type=jnp.float32)
    return jax.nn.silu(embedded + time_features(times)).astype(jnp.bfloat16)

def modulation(cond, weight):
    return jnp.einsum('nd,dkf->nkf', cond.astype(jnp.float32), weight.astype(jnp.float32), precision=lax.Precision.HIGHEST)

def positions():
    quarter = D // 4
    omega = 1.0 / 10000.0 ** (jnp.arange(quarter, dtype=jnp.float32) / quarter)
    side = math.isqrt(SEQ)
    cells = jnp.arange(SEQ, dtype=jnp.int32)
    grid_row = (cells // side).astype(jnp.float32)
    grid_col = (cells % side).astype(jnp.float32)
    row_angle = grid_row[:, None] * omega[None, :]
    col_angle = grid_col[:, None] * omega[None, :]
    return jnp.concatenate([jnp.sin(row_angle), jnp.cos(row_angle), jnp.sin(col_angle), jnp.cos(col_angle)], axis=1)

def layer_norm(values):
    center = values - lax.optimization_barrier(jnp.mean(values, axis=-1, keepdims=True))
    spread = lax.optimization_barrier(jnp.mean(center * center, axis=-1, keepdims=True))
    reciprocal = lax.rsqrt(spread + 1e-06)
    return (center * reciprocal, reciprocal)

def gelu_slope(pre):
    inner = ROOT_TWO_PI * (pre + 0.044715 * pre * pre * pre)
    tangent = jnp.tanh(inner)
    return 0.5 * (1.0 + tangent) + 0.5 * pre * (1.0 - tangent * tangent) * ROOT_TWO_PI * (1.0 + 3.0 * 0.044715 * pre * pre)

def contract_last(left, right):
    return lax.dot_general(left, right, (((1,), (1,)), ((), ())), preferred_element_type=jnp.float32)

def contract_first(left, right):
    return lax.dot_general(left, right, (((0,), (0,)), ((), ())), preferred_element_type=jnp.float32)

def network(state, mods, patch_weight, up_weight, down_weight, out_weight, pos):
    samples = state.shape[0]
    tokens = state.reshape(samples * SEQ, PATCH).astype(jnp.bfloat16)
    base = jnp.dot(tokens, patch_weight, preferred_element_type=jnp.float32).reshape(samples, SEQ, D) + pos[None]
    shift = mods[:, 0][:, None, :]
    scale = mods[:, 1][:, None, :]
    gate = mods[:, 2][:, None, :]
    normed, _ = layer_norm(base)
    act = (normed * (1.0 + scale) + shift).astype(jnp.bfloat16).reshape(samples * SEQ, D)
    pre = jnp.dot(act, up_weight, preferred_element_type=jnp.float32)
    hidden = jax.nn.gelu(pre, approximate=True).astype(jnp.bfloat16)
    width = FF // N_COL
    mixed = jnp.zeros((samples * SEQ, D), jnp.float32)
    for column in range(N_COL):
        part = contract_last(hidden[:, column * width:(column + 1) * width], down_weight[:, column * width:(column + 1) * width])
        rounded = lax.optimization_barrier(part.astype(jnp.bfloat16))
        mixed = mixed + rounded.astype(jnp.float32)
    later = base + gate * mixed.reshape(samples, SEQ, D)
    final, reciprocal = layer_norm(later)
    velocity = contract_last(final.astype(jnp.bfloat16).reshape(samples * SEQ, D), out_weight)
    return (velocity.reshape(samples, SEQ * PATCH // 128, 128), (act, pre, hidden, final, reciprocal, gate))

def reference(latents, labels, step_index, seeds, class_table, teacher_patch, teacher_mod, teacher_up, teacher_down, teacher_out, student_patch, student_mod, student_up, student_down, student_out):
    block = 8
    count = BATCH // block
    pos = positions()

    def one_block(carry, inputs):
        clean, names, steps, keys = inputs
        now = steps.astype(jnp.float32) / STEPS
        middle = now - 0.5 / STEPS
        ending = now - 1.0 / STEPS
        alpha, sigma = plan(now[:, None, None])
        alpha_mid, sigma_mid = plan(middle[:, None, None])
        alpha_end, sigma_end = plan(ending[:, None, None])
        cond_now = condition(now, names, class_table)
        cond_mid = condition(middle, names, class_table)
        teacher_now = modulation(cond_now, teacher_mod)
        teacher_mid = modulation(cond_mid, teacher_mod)
        student_mods = modulation(cond_now, student_mod)
        noisy = alpha * clean + sigma * noise_of(keys)
        first_v, _ = network(noisy, teacher_now, teacher_patch, teacher_up, teacher_down, teacher_out, pos)
        first_x = alpha * noisy - sigma * first_v
        halfway = alpha_mid * first_x + sigma_mid * (noisy - alpha * first_x) / sigma
        second_v, _ = network(halfway, teacher_mid, teacher_patch, teacher_up, teacher_down, teacher_out, pos)
        second_x = alpha_mid * halfway - sigma_mid * second_v
        landing = alpha_end * second_x + sigma_end * (halfway - alpha_mid * second_x) / sigma_mid
        ratio = sigma_end / sigma
        target = (landing - ratio * noisy) / (alpha_end - ratio * alpha)
        student_v, saved = network(noisy, student_mods, student_patch, student_up, student_down, student_out, pos)
        student_x = alpha * noisy - sigma * student_v
        weight = jnp.maximum(alpha * alpha / (sigma * sigma), 1.0)
        back_velocity = (-2.0 * sigma * weight * (student_x - target) / BATCH).reshape(block * SEQ, PATCH)
        act, pre, hidden, final, reciprocal, gate = saved
        back_final = jnp.dot(back_velocity, student_out.astype(jnp.float32), precision=lax.Precision.HIGHEST).reshape(block, SEQ, D)
        centre = lax.optimization_barrier(jnp.mean(back_final, axis=2, keepdims=True))
        along = lax.optimization_barrier(jnp.mean(back_final * final, axis=2, keepdims=True))
        back_mixed = (gate * (reciprocal * (back_final - centre - final * along))).astype(jnp.bfloat16).reshape(block * SEQ, D)
        down_term = contract_first(back_mixed, hidden)
        back_hidden = jnp.dot(back_mixed, student_down, preferred_element_type=jnp.float32)
        back_pre = (back_hidden * gelu_slope(pre)).astype(jnp.bfloat16)
        up_term = contract_first(act, back_pre)
        return ((carry[0] + up_term, carry[1] + down_term), None)
    inputs = (latents.reshape(count, block, SEQ * PATCH // 128, 128), labels.reshape(count, block), step_index.reshape(count, block), seeds.reshape(count, block))
    zeros = jnp.zeros((D, FF), jnp.float32)
    (up_gradient, down_gradient), _ = lax.scan(one_block, (zeros, zeros), inputs)
    return (up_gradient, down_gradient)
```

```python
import math

import jax
import jax.numpy as jnp
import numpy as np
from jax import lax
from jax.experimental import pallas as pl
from jax.experimental.pallas import tpu as pltpu
from jax.sharding import PartitionSpec as P

D = 1152
CLASSES = 1000
SEQ = 256
PATCH = 16
STEPS = 8


HALF_PI = 0.5 * math.pi
ROOT_TWO_PI = math.sqrt(2.0 / math.pi)


def plan(times):
    return (jnp.cos(HALF_PI * times), jnp.sin(HALF_PI * times))


def mixing(value):
    amount = jnp.int32(16)
    value = value ^ lax.shift_right_logical(value, amount)
    value = value * 73244475
    value = value ^ lax.shift_right_logical(value, amount)
    value = value * 73244475
    value = value ^ lax.shift_right_logical(value, amount)
    return value


def noise_of(seeds):
    total = SEQ * PATCH
    places = jnp.arange(total, dtype=jnp.int32).reshape(1, total // 128, 128)
    mixed = mixing(seeds[:, None, None] * 1103515245 + places * 40503 + 12345)
    uniform = (lax.shift_right_logical(mixed, jnp.int32(8)).astype(jnp.float32) + 0.5) * (
        1.0 / 16777216.0
    )
    return math.sqrt(2.0) * lax.erf_inv(2.0 * uniform - 1.0)


def time_features(times):
    half = D // 2
    freqs = jnp.exp(-math.log(10000.0) * jnp.arange(half, dtype=jnp.float32) / half)
    angle = (1000.0 * times)[:, None] * freqs[None, :]
    return jnp.concatenate([jnp.cos(angle), jnp.sin(angle)], axis=1)


def condition(times, labels, class_table):
    onehot = (labels[:, None] == jnp.arange(CLASSES, dtype=jnp.int32)[None, :]).astype(jnp.bfloat16)
    embedded = jnp.dot(onehot, class_table, preferred_element_type=jnp.float32)
    return jax.nn.silu(embedded + time_features(times)).astype(jnp.bfloat16)


def positions():
    quarter = D // 4
    omega = 1.0 / 10000.0 ** (jnp.arange(quarter, dtype=jnp.float32) / quarter)
    side = math.isqrt(SEQ)
    cells = jnp.arange(SEQ, dtype=jnp.int32)
    grid_row = (cells // side).astype(jnp.float32)
    grid_col = (cells % side).astype(jnp.float32)
    row_angle = grid_row[:, None] * omega[None, :]
    col_angle = grid_col[:, None] * omega[None, :]
    return jnp.concatenate(
        [jnp.sin(row_angle), jnp.cos(row_angle), jnp.sin(col_angle), jnp.cos(col_angle)], axis=1
    )


def layer_norm(values):
    center = values - jnp.mean(values, axis=-1, keepdims=True)
    spread = jnp.mean(center * center, axis=-1, keepdims=True)
    reciprocal = lax.rsqrt(spread + 1e-06)
    return (center * reciprocal, reciprocal)


def gelu_slope(pre):
    inner = ROOT_TWO_PI * (pre + 0.044715 * pre * pre * pre)
    tangent = jnp.tanh(inner)
    return 0.5 * (1.0 + tangent) + 0.5 * pre * (1.0 - tangent * tangent) * ROOT_TWO_PI * (
        1.0 + 3.0 * 0.044715 * pre * pre
    )


def contract_last(left, right):
    return lax.dot_general(
        left, right, (((1,), (1,)), ((), ())), preferred_element_type=jnp.float32
    )


def contract_first(left, right):
    return lax.dot_general(
        left, right, (((0,), (0,)), ((), ())), preferred_element_type=jnp.float32
    )


def modulate(base, mods):
    normed, _ = layer_norm(base)
    shift = mods[0][None, :, None, :]
    scale = mods[1][None, :, None, :]
    return (normed * (1.0 + scale) + shift).astype(jnp.bfloat16).reshape(-1, D)


def embed(tokens, patch_weight, pos):
    flat = tokens.reshape(-1, PATCH)
    product = jnp.dot(flat, patch_weight, preferred_element_type=jnp.float32)
    return product.reshape(*tokens.shape[:-1], D) + pos


def scatter_columns(partial_out, groups):
    blocks = partial_out.reshape(groups, -1, D)
    swapped = lax.all_to_all(blocks, "col", split_axis=0, concat_axis=0, tiled=True)
    return jnp.sum(swapped.astype(jnp.float32), axis=0)


def reduce_gradient(left, right, group):
    names = ("dp", "row")
    me = lax.axis_index(names)
    pairs = group // 2
    mine, parity = me // 2, me % 2
    partial = contract_first(left, right)
    blocks = partial.reshape(pairs, 2, partial.shape[0] // group, partial.shape[1])
    keep = lax.dynamic_index_in_dim(blocks, parity, 1, keepdims=False)
    give = lax.dynamic_index_in_dim(blocks.astype(jnp.bfloat16), 1 - parity, 1, keepdims=False)
    got = lax.ppermute(give, names, [(i, i ^ 1) for i in range(group)])
    pair = keep + got.astype(jnp.float32)
    sent = pair.astype(jnp.bfloat16)
    total = lax.dynamic_index_in_dim(pair, mine, 0, keepdims=False)
    for step in range(1, pairs):
        piece = lax.dynamic_index_in_dim(sent, (mine + step) % pairs, 0, keepdims=False)
        hop = [(i, (i + 2 * step) % group) for i in range(group)]
        total = total + lax.ppermute(piece, names, hop).astype(jnp.float32)
    return total


def body(
    latents,
    labels,
    step_index,
    seeds,
    class_table,
    teacher_patch,
    teacher_mod,
    teacher_up,
    teacher_down,
    teacher_out,
    student_patch,
    student_mod,
    student_up,
    student_down,
    student_out,
):
    samples = latents.shape[0]
    group = lax.axis_size(("dp", "row"))
    groups = lax.axis_size("col")
    column = lax.axis_index("col")
    chunk = SEQ // groups
    batch_total = samples * group
    up_panel, down_panel, student_up_panel, student_panel = [
        lax.all_gather(weight, ("dp", "row"), axis=0, tiled=True)
        for weight in (teacher_up, teacher_down, student_up, student_down)
    ]
    both = lax.all_gather(jnp.stack([labels, step_index]), ("dp", "row"), axis=1, tiled=True)
    all_labels, all_steps = both[0], both[1]
    all_now = all_steps.astype(jnp.float32) / STEPS
    cond = condition(
        jnp.concatenate([all_now, all_now - 0.5 / STEPS]),
        jnp.concatenate([all_labels, all_labels]),
        class_table,
    )
    own_rows = teacher_mod.shape[0]
    offset = lax.axis_index(("dp", "row")) * own_rows
    rows = lax.dynamic_slice_in_dim(cond, offset, own_rows, 1)
    width = teacher_mod.shape[2]
    parts = []
    for taken, weights in ((2, teacher_mod), (1, student_mod)):
        for index in range(3):
            product = jnp.dot(
                rows[: taken * batch_total],
                weights[:, index],
                preferred_element_type=jnp.float32,
            ).reshape(taken, group, samples, width)
            parts.extend(product[which] for which in range(taken))
    parts = jnp.concatenate(parts, axis=1)
    swapped = lax.all_to_all(parts, ("dp", "row"), split_axis=0, concat_axis=0, tiled=True)
    sums = jnp.sum(swapped, axis=0)
    gathered = lax.all_gather(sums, "col", axis=0, tiled=False)
    joined = jnp.concatenate([gathered[place] for place in range(groups)], axis=-1)

    def entry(place):
        return joined[place * samples : (place + 1) * samples]

    teacher_now = [entry(2 * index) for index in range(3)]
    teacher_mid = [entry(2 * index + 1) for index in range(3)]
    student_mods = [entry(6 + index) for index in range(3)]

    now = step_index.astype(jnp.float32) / STEPS
    alpha, sigma = plan(now[:, None, None])
    alpha_mid, sigma_mid = plan((now - 0.5 / STEPS)[:, None, None])
    alpha_end, sigma_end = plan((now - 1.0 / STEPS)[:, None, None])
    noisy_full = alpha * latents + sigma * noise_of(seeds)
    noisy_full = noisy_full.reshape(samples, groups, chunk, PATCH).transpose(1, 0, 2, 3)
    noisy = lax.dynamic_index_in_dim(noisy_full, column, 0, keepdims=False)
    noisy_tokens = noisy_full.astype(jnp.bfloat16)
    pos = positions().reshape(groups, 1, chunk, D)
    own_pos = lax.dynamic_index_in_dim(pos, column, 0, keepdims=True)

    def own_output(own_base, gate, mixed, out_weight):
        later = own_base[0] + gate[:, None, :] * mixed.reshape(samples, chunk, D)
        final, _ = layer_norm(later)
        velocity = contract_last(final.astype(jnp.bfloat16).reshape(-1, D), out_weight)
        return velocity.reshape(samples, chunk, PATCH)

    def teacher(tokens, own_tokens, these):
        act = modulate(embed(tokens, teacher_patch, pos), these)
        pre = jnp.dot(act, up_panel, preferred_element_type=jnp.float32)
        hidden = jax.nn.gelu(pre, approximate=True).astype(jnp.bfloat16)
        mixed = scatter_columns(contract_last(hidden, down_panel).astype(jnp.bfloat16), groups)
        own_base = embed(own_tokens[None], teacher_patch, own_pos)
        return own_output(own_base, these[2], mixed, teacher_out)

    first_v = teacher(noisy_tokens, noisy.astype(jnp.bfloat16), teacher_now)
    first_x = alpha * noisy - sigma * first_v
    halfway = alpha_mid * first_x + sigma_mid * (noisy - alpha * first_x) / sigma
    halfway_own = halfway.astype(jnp.bfloat16)
    halfway_tokens = lax.all_gather(halfway_own, "col", axis=0, tiled=False)
    gate = student_mods[2]
    base = embed(noisy_tokens, student_patch, pos)
    act = modulate(base, student_mods)
    pre = jnp.dot(act, student_up_panel, preferred_element_type=jnp.float32)
    hidden = jax.nn.gelu(pre, approximate=True).astype(jnp.bfloat16)
    hidden, halfway_tokens = lax.optimization_barrier((hidden, halfway_tokens))
    second_v = teacher(halfway_tokens, halfway_own, teacher_mid)
    second_x = alpha_mid * halfway - sigma_mid * second_v
    landing = alpha_end * second_x + sigma_end * (halfway - alpha_mid * second_x) / sigma_mid
    ratio = sigma_end / sigma
    target = (landing - ratio * noisy) / (alpha_end - ratio * alpha)

    own_mixed = scatter_columns(contract_last(hidden, student_panel).astype(jnp.bfloat16), groups)
    own_base = embed(noisy.astype(jnp.bfloat16)[None], student_patch, own_pos)[0]
    later = own_base + gate[:, None, :] * own_mixed.reshape(samples, chunk, D)
    final, reciprocal = layer_norm(later)
    student_v = contract_last(final.astype(jnp.bfloat16).reshape(-1, D), student_out)
    student_x = alpha * noisy - sigma * student_v.reshape(samples, chunk, PATCH)
    weight = jnp.maximum(alpha * alpha / (sigma * sigma), 1.0)
    back_velocity = -2.0 * sigma * weight * (student_x - target) / batch_total
    back_final = jnp.dot(
        back_velocity.reshape(-1, PATCH),
        student_out.astype(jnp.float32),
        precision=lax.Precision.HIGHEST,
    ).reshape(samples, chunk, D)
    centre = jnp.mean(back_final, axis=2, keepdims=True)
    along = jnp.mean(back_final * final, axis=2, keepdims=True)
    own_back = (
        gate[:, None, :] * (reciprocal * (back_final - centre - final * along))
    ).astype(jnp.bfloat16)
    back_mixed = lax.all_gather(own_back.reshape(-1, D), "col", axis=0, tiled=True)
    back_hidden = jnp.dot(back_mixed, student_panel, preferred_element_type=jnp.float32)
    back_pre = (back_hidden * gelu_slope(pre)).astype(jnp.bfloat16)
    down_gradient = reduce_gradient(back_mixed, hidden, group)
    up_gradient = reduce_gradient(act, back_pre, group)
    return (up_gradient, down_gradient)


TILE = 128
BLOCK = 384
MESH = pl.DeviceIdType.MESH


def ln_parts(values):
    center = values - jnp.mean(values, axis=-1, keepdims=True)
    spread = jnp.mean(center * center, axis=-1, keepdims=True)
    reciprocal = lax.rsqrt(spread + 1e-06)
    return center * reciprocal, reciprocal


def position_tables():
    quarter = D // 4
    side = math.isqrt(SEQ)
    omega = 1.0 / 10000.0 ** (np.arange(quarter, dtype=np.float32) / np.float32(quarter))
    angle = np.arange(side, dtype=np.float32)[:, None] * omega[None, :].astype(np.float32)
    table = np.concatenate([np.sin(angle), np.cos(angle)], axis=1).astype(np.float32)
    blank = np.zeros_like(table)
    return np.stack(
        [np.concatenate([table, blank], axis=1), np.concatenate([blank, table], axis=1)]
    )


def fused_kernel(sizes, *refs):
    spread_rows, line, samples, rows = sizes
    (nz, coef, cond, tmod, smod, tabs, pt, ps, ot, os_, tup, tdn, sup, sdn) = refs[:14]
    ug, dg = refs[14:16]
    (
        wtu, wtd, wsu, wsd, condall, mpart, mrecv, msum, modb,
        actt, acts, hidt, hids, pres, part, recv, mixed, recip, half, vstu, target,
        back, full, bpre, ugrad, dgrad, pairu, paird, sendu, sendd, crossu, crossd,
        loc, wcs, wcr, wss, wsr, cs, cr, ms, mr, zs, zr, ls, lr, hs, hr, bs, br, gps, gpr, gcs, gcr,
    ) = refs[16:]
    chips = 4
    group = 2 * chips
    tiles = 2 * samples
    blocks = D // BLOCK
    chunks = samples * blocks
    span = samples * TILE
    far = line - 1
    dp, row, col = lax.axis_index("dp"), lax.axis_index("row"), lax.axis_index("col")
    me = dp * spread_rows + row
    chip, core = me // 2, me % 2
    sib = 2 * chip + 1 - core

    def member(index):
        return {"dp": index // spread_rows, "row": index % spread_rows}

    def chip_at(offset):
        return (chip + offset) % chips

    def remote(src, dst, send, recv_sem, where):
        return pltpu.make_async_remote_copy(
            src_ref=src, dst_ref=dst, send_sem=send, recv_sem=recv_sem,
            device_id=where, device_id_type=MESH,
        )

    barrier = pltpu.get_barrier_semaphore()
    for offset in range(1, group):
        pl.semaphore_signal(barrier, inc=1, device_id=member((me + offset) % group), device_id_type=MESH)
    for offset in range(1, line):
        pl.semaphore_signal(barrier, inc=1, device_id={"col": (col + offset) % line}, device_id_type=MESH)
    pl.semaphore_wait(barrier, group - 1 + line - 1)

    def slot(panel, index):
        return panel.at[pl.ds(pl.multiple_of(index * rows, 16), rows), :]

    panels = (wtu, wtd, wsu, wsd)

    def fetch(w, shard):
        return pltpu.make_async_copy(shard, slot(panels[w], me), loc.at[w])

    def cross(w, offset):
        own = slot(panels[w], me)
        return remote(own, own, wcs.at[w, offset - 1], wcr.at[w, offset - 1],
                      member(2 * chip_at(offset) + core))

    def aside(w, offset):
        held = slot(panels[w], 2 * chip_at(chips - offset) + core)
        return remote(held, held, wss.at[w, offset], wsr.at[w, offset], member(sib))

    def cond_copy(offset):
        return remote(cond.at[(me + offset) % group], condall.at[me], cs.at[offset - 1], cr.at[offset - 1],
                      member((me + offset) % group))

    def mod_copy(offset):
        return remote(mpart.at[(me + offset) % group], mrecv.at[offset - 1], ms.at[offset - 1], mr.at[offset - 1],
                      member((me + offset) % group))

    def line_copy(offset):
        return remote(msum.at[col], msum.at[col], zs.at[offset - 1], zr.at[offset - 1],
                      {"col": (col + offset) % line})

    for w, shard in enumerate((tup, tdn, sup, sdn)):
        fetch(w, shard).start()
    for offset in range(1, group):
        cond_copy(offset).start()
    condall[me] = cond[me]
    fetch(0, tup).wait()
    cross(0, 2).start()
    aside(0, 0).start()
    for offset in range(1, group):
        cond_copy(offset).wait()
    lhs = condall[...].reshape(group * 8, rows).astype(jnp.bfloat16)
    for place in range(3):
        for base, weights in ((0, tmod), (3, smod)):
            product = jnp.dot(lhs, weights[place], preferred_element_type=jnp.float32)
            width = product.shape[1]
            mpart[:, base + place] = product.reshape(group, 8, width)
    for offset in range(1, group):
        mod_copy(offset).start()
    cross(0, 1).start()
    cross(0, 3).start()
    for w, shard in ((1, tdn), (2, sup), (3, sdn)):
        fetch(w, shard).wait()
        for offset in (2, 1, 3):
            cross(w, offset).start()
        aside(w, 0).start()
    total = mpart[me]
    for offset in range(1, group):
        mod_copy(offset).wait()
        total = total + mrecv[offset - 1]
    msum[col] = total
    for offset in range(1, line):
        line_copy(offset).start()
    for offset in range(1, line):
        line_copy(offset).wait()
    width = tmod.shape[2]
    for place in range(line):
        for entry in range(6):
            modb[entry, :, place * width : (place + 1) * width] = msum[place, entry]

    def place_of(h):
        rows_of = tabs[0, pl.ds(pl.multiple_of(h * 8, 8), 8), :]
        side = SEQ // 16
        grid = jnp.broadcast_to(rows_of[:, None, :], (8, side, D)) + tabs[1][None]
        return grid.reshape(TILE, D)

    def base_of(tokens, patch, h):
        flat = tokens.T.astype(jnp.bfloat16)
        return jnp.dot(flat, patch[...], preferred_element_type=jnp.float32) + place_of(h)

    def lanes(index):
        return pl.ds(pl.multiple_of(index * TILE, TILE), TILE)

    def stripe(index):
        return pl.ds(pl.multiple_of(index * BLOCK, BLOCK), BLOCK)

    def act_tiles(state, patch, first, shift_row, out):
        def step(i, carry):
            h, s = i // samples, i % samples
            base = base_of(state(h, s), patch, h)
            normed, _ = ln_parts(base)
            shift = modb[first, pl.ds(shift_row + s, 1), :]
            scale = modb[first + 1, pl.ds(shift_row + s, 1), :]
            out[lanes(i), :] = (normed * (1.0 + scale) + shift).astype(jnp.bfloat16)
            return carry

        lax.fori_loop(0, tiles, step, 0)

    def up_tiles(act, panel, hidden, keep):
        def step(i, carry):
            h, n = i // blocks, i % blocks
            pre = jnp.dot(act[stripe(h), :], panel[:, stripe(n)], preferred_element_type=jnp.float32)
            if keep is not None:
                keep[stripe(h), stripe(n)] = pre
            hidden[stripe(h), stripe(n)] = jax.nn.gelu(pre, approximate=True).astype(jnp.bfloat16)
            return carry

        lax.fori_loop(0, 2 * blocks, step, 0)

    def hop_of(h):
        return h * col + (1 - h) * (far - col)

    def chunk_copy(h, j):
        return remote(part.at[h, j], recv.at[h, j], ls.at[h, j], lr.at[h, j], {"col": col + 2 * h - 1})

    def down_tiles(hidden, panel, first):
        near = 1 - (2 * col) // line

        def step(i, carry):
            turn, f = i // blocks, i % blocks
            h = near * (1 - turn) + (1 - near) * turn
            product = contract_last(hidden[stripe(h), :], panel[stripe(f), :]).astype(jnp.bfloat16)
            for s in range(samples):
                part[h, first + s * blocks + f] = product[s * TILE : (s + 1) * TILE]
            return carry

        lax.fori_loop(0, blocks, step, 0)
        for h in (1, 0):
            @pl.when(hop_of(h) == 0)
            def _():
                def send(j, carry):
                    chunk_copy(h, first + j).start()
                    return carry

                lax.fori_loop(0, chunks, send, 0)

        lax.fori_loop(blocks, 2 * blocks, step, 0)

    def line_steps(first, count, start, stop):
        def step(t, carry):
            for h in (1, 0):
                hop = hop_of(h)
                j = t - 2 * hop

                @pl.when((hop > 0) & (j >= 0) & (j < count))
                def _():
                    c = first + j
                    chunk_copy(h, c).wait_recv()
                    sum_ = part[h, c].astype(jnp.float32) + recv[h, c].astype(jnp.float32)

                    @pl.when(hop < far)
                    def _():
                        part[h, c] = sum_.astype(jnp.bfloat16)
                        chunk_copy(h, c).start()

                    @pl.when(hop == far)
                    def _():
                        mixed[c] = sum_

            return carry

        lax.fori_loop(start, stop, step, 0)

    def drain(first):
        for h in (1, 0):
            @pl.when(hop_of(h) < far)
            def _():
                def end(j, carry):
                    chunk_copy(h, first + j).wait_send()
                    return carry

                lax.fori_loop(0, chunks, end, 0)

    def collect(w):
        for offset in (2, 1, 3):
            cross(w, offset).wait_recv()
            aside(w, offset).start()
        for offset in range(chips):
            aside(w, offset).wait_recv()

    owner = (col == 0) | (col == far)
    mine = col // far

    def later_of(tokens, patch, first_chunk, s, gate):
        sums = [mixed[first_chunk + s * blocks + f] for f in range(blocks)]
        return base_of(tokens, patch, mine) + gate * jnp.concatenate(sums, axis=1)

    def velocity_of(final, out):
        return contract_last(out[...], final.astype(jnp.bfloat16))

    def row_of(index, s):
        return coef[index : index + 1, lanes(s)]

    def noisy_of(h, s):
        return nz[:, lanes(h * samples + s)]

    def half_of(h, s):
        return half[h, :, lanes(s)]

    def half_copy(offset):
        return remote(half.at[mine], half.at[mine], hs.at[offset - 1], hr.at[mine, offset - 1],
                      {"col": (col + offset) % line})

    act_tiles(noisy_of, pt, 0, 0, actt)
    collect(0)
    up_tiles(actt, wtu, hidt, None)
    act_tiles(noisy_of, ps, 3, 0, acts)
    collect(1)
    down_tiles(hidt, wtd, 0)
    steps = chunks + 2 * far
    line_steps(0, chunks, 0, steps)

    @pl.when(owner)
    def _():
        def step(s, carry):
            noisy = noisy_of(mine, s)
            final, _ = ln_parts(later_of(noisy, pt, 0, s, modb[2, pl.ds(s, 1), :]))
            speed = velocity_of(final, ot)
            alpha, sigma, alpha_mid, sigma_mid = [row_of(index, s) for index in range(4)]
            first_x = alpha * noisy - sigma * speed
            half[mine, :, lanes(s)] = alpha_mid * first_x + sigma_mid * (noisy - alpha * first_x) / sigma
            return carry

        lax.fori_loop(0, samples, step, 0)
        for offset in range(1, line):
            half_copy(offset).start()

    collect(2)
    up_tiles(acts, wsu, hids, pres)
    drain(0)
    for h in range(2):
        source = h * far

        @pl.when(col != source)
        def _():
            for offset in range(1, line):
                @pl.when((source + offset) % line == col)
                def _():
                    remote(half.at[h], half.at[h], hs.at[offset - 1], hr.at[h, offset - 1], {"col": source}).wait_recv()

    act_tiles(half_of, pt, 0, samples, actt)
    up_tiles(actt, wtu, hidt, None)
    down_tiles(hidt, wtd, 0)
    line_steps(0, chunks, 0, 2)
    collect(3)
    down_tiles(hids, wsd, chunks)
    line_steps(0, 2 * chunks, 2, steps)

    @pl.when(owner)
    def _():
        def step(s, carry):
            noisy, middle = noisy_of(mine, s), half_of(mine, s)
            final, _ = ln_parts(later_of(middle, pt, 0, s, modb[2, pl.ds(samples + s, 1), :]))
            speed = velocity_of(final, ot)
            alpha, sigma, alpha_mid, sigma_mid, alpha_end, sigma_end = [row_of(index, s) for index in range(6)]
            second_x = alpha_mid * middle - sigma_mid * speed
            landing = alpha_end * second_x + sigma_end * (middle - alpha_mid * second_x) / sigma_mid
            ratio = sigma_end / sigma
            target[:, lanes(s)] = (landing - ratio * noisy) / (alpha_end - ratio * alpha)
            return carry

        lax.fori_loop(0, samples, step, 0)

    line_steps(0, 2 * chunks, steps, steps + chunks)

    def back_copy(h, j):
        return remote(back.at[h, j], back.at[h, j], bs.at[h, j], br.at[h, j], {"col": col + 1 - 2 * h})

    def tile_rows(h, s):
        return pl.ds(pl.multiple_of((h * samples + s) * TILE, TILE), TILE)

    @pl.when(owner)
    def _():
        def step(s, carry):
            noisy = noisy_of(mine, s)
            gate = modb[5, pl.ds(s, 1), :]
            final, reciprocal = ln_parts(later_of(noisy, ps, chunks, s, gate))
            speed = velocity_of(final, os_)
            alpha, sigma = row_of(0, s), row_of(1, s)
            student_x = alpha * noisy - sigma * speed
            weight = jnp.maximum(alpha * alpha / (sigma * sigma), 1.0)
            speed_back = -2.0 * sigma * weight * (student_x - target[:, lanes(s)]) / (samples * group)
            high = speed_back.astype(jnp.bfloat16).astype(jnp.float32)
            rest = speed_back - high
            middle = rest.astype(jnp.bfloat16).astype(jnp.float32)
            low = rest - middle
            pieces = jnp.concatenate([high, middle, low], axis=0).T.astype(jnp.bfloat16)
            outs = jnp.concatenate([os_[...]] * 3, axis=0)
            back_final = jnp.dot(pieces, outs, preferred_element_type=jnp.float32)
            centre = jnp.mean(back_final, axis=-1, keepdims=True)
            along = jnp.mean(back_final * final, axis=-1, keepdims=True)
            own = (gate * (reciprocal * (back_final - centre - final * along))).astype(jnp.bfloat16)
            full[tile_rows(mine, s), :] = own
            for f in range(blocks):
                back[mine, s * blocks + f] = own[:, f * BLOCK : (f + 1) * BLOCK]
            for f in range(blocks):
                back_copy(mine, s * blocks + f).start()
            return carry

        lax.fori_loop(0, samples, step, 0)

    def relay(t, carry):
        for h in (0, 1):
            hop = far - hop_of(h)
            j = t - 2 * hop

            @pl.when((hop > 0) & (j >= 0) & (j < chunks))
            def _():
                back_copy(h, j).wait_recv()

                @pl.when(hop < far)
                def _():
                    back_copy(h, j).start()

                full[tile_rows(h, j // blocks), stripe(j % blocks)] = back[h, j]

        return carry

    lax.fori_loop(0, steps, relay, 0)

    def pair_copy(grad, landing, which, offset):
        block = 2 * chip_at(offset) + 1 - core
        source = grad.at[pl.ds(pl.multiple_of(block * rows, 8), rows), :]
        return remote(source, landing.at[offset], gps.at[which, offset], gpr.at[which, offset], member(sib))

    def grad_copy(staged, landing, which, offset):
        return remote(staged.at[offset - 1], landing.at[offset - 1], gcs.at[which, offset - 1],
                      gcr.at[which, offset - 1], member(2 * chip_at(offset) + core))

    def own_rows(grad, offset):
        block = 2 * chip_at(offset) + core
        return grad[pl.ds(pl.multiple_of(block * rows, 8), rows), :]

    def outer(left, right, grad):
        def step(i, carry):
            r, n = i // blocks, i % blocks
            grad[stripe(r), stripe(n)] = contract_first(left[:, stripe(r)], right[:, stripe(n)])
            return carry

        lax.fori_loop(0, blocks * blocks, step, 0)

    def pair_start(grad, landing, which):
        for offset in (2, 1, 3, 0):
            pair_copy(grad, landing, which, offset).start()

    def cross_start(grad, landing, staged, received, which):
        for offset in (2, 1, 3):
            pair_copy(grad, landing, which, offset).wait_recv()
            staged[offset - 1] = (own_rows(grad, offset) + landing[offset]).astype(jnp.bfloat16)
            grad_copy(staged, received, which, offset).start()

    def finish(grad, landing, staged, received, which, out):
        pair_copy(grad, landing, which, 0).wait_recv()
        sum_ = own_rows(grad, 0) + landing[0]
        for offset in (2, 1, 3):
            grad_copy(staged, received, which, offset).wait_recv()
            sum_ = sum_ + received[offset - 1].astype(jnp.float32)
        out[...] = sum_
        for offset in (2, 1, 3):
            grad_copy(staged, received, which, offset).wait_send()
        for offset in range(chips):
            pair_copy(grad, landing, which, offset).wait_send()

    outer(full, hids, dgrad)
    pair_start(dgrad, paird, 0)

    def back_step(i, carry):
        h, n = i // blocks, i % blocks
        hidden_back = jnp.dot(full[stripe(h), :], wsd[:, stripe(n)], preferred_element_type=jnp.float32)
        bpre[stripe(h), stripe(n)] = (hidden_back * gelu_slope(pres[stripe(h), stripe(n)])).astype(jnp.bfloat16)
        return carry

    lax.fori_loop(0, 2 * blocks, back_step, 0)
    cross_start(dgrad, paird, sendd, crossd, 0)
    outer(acts, bpre, ugrad)
    pair_start(ugrad, pairu, 1)
    cross_start(ugrad, pairu, sendu, crossu, 1)
    finish(dgrad, paird, sendd, crossd, 0, dg)
    finish(ugrad, pairu, sendu, crossu, 1, ug)

    drain(0)
    drain(chunks)
    for h in (0, 1):
        @pl.when(far - hop_of(h) < far)
        def _():
            def end(j, carry):
                back_copy(h, j).wait_send()
                return carry

            lax.fori_loop(0, chunks, end, 0)

    @pl.when(owner)
    def _():
        for offset in range(1, line):
            half_copy(offset).wait_send()

    for w in range(4):
        for offset in range(1, chips):
            cross(w, offset).wait_send()
        for offset in range(chips):
            aside(w, offset).wait_send()


def fused_call(mesh, operands):
    samples = operands[0].shape[1] // SEQ
    line = mesh.shape["col"]
    rows, hidden = operands[10].shape
    width = operands[3].shape[2]
    chips, group = 4, 8
    tokens = samples * SEQ
    chunks = samples * (D // BLOCK)
    f32, bf16 = jnp.float32, jnp.bfloat16
    vmem, dma = pltpu.VMEM, pltpu.SemaphoreType.DMA
    scratch = [vmem((D, hidden), bf16)] * 4 + [
        vmem((group, 8, rows), f32),
        vmem((group, 6, 8, width), f32),
        vmem((group - 1, 6, 8, width), f32),
        vmem((line, 6, 8, width), f32),
        vmem((6, 8, D), f32),
        vmem((tokens, D), bf16),
        vmem((tokens, D), bf16),
        vmem((tokens, hidden), bf16),
        vmem((tokens, hidden), bf16),
        vmem((tokens, hidden), f32),
        vmem((2, 2 * chunks, TILE, BLOCK), bf16),
        vmem((2, 2 * chunks, TILE, BLOCK), bf16),
        vmem((2 * chunks, TILE, BLOCK), f32),
        vmem((8, 128), f32),
        vmem((2, PATCH, samples * TILE), f32),
        vmem((8, 128), f32),
        vmem((PATCH, samples * TILE), f32),
        vmem((2, chunks, TILE, BLOCK), bf16),
        vmem((tokens, D), bf16),
        vmem((tokens, hidden), bf16),
        vmem((D, hidden), f32),
        vmem((D, hidden), f32),
        vmem((chips, rows, hidden), f32),
        vmem((chips, rows, hidden), f32),
        vmem((chips - 1, rows, hidden), bf16),
        vmem((chips - 1, rows, hidden), bf16),
        vmem((chips - 1, rows, hidden), bf16),
        vmem((chips - 1, rows, hidden), bf16),
        dma((4,)),
        dma((4, chips - 1)), dma((4, chips - 1)), dma((4, chips)), dma((4, chips)),
        dma((group - 1,)), dma((group - 1,)), dma((group - 1,)), dma((group - 1,)),
        dma((line - 1,)), dma((line - 1,)),
        dma((2, 2 * chunks)), dma((2, 2 * chunks)),
        dma((line - 1,)), dma((2, line - 1)),
        dma((2, chunks)), dma((2, chunks)),
        dma((2, chips)), dma((2, chips)), dma((2, chips - 1)), dma((2, chips - 1)),
    ]

    def kernel(*refs):
        fused_kernel((mesh.shape["row"], line, samples, rows), *refs)

    specs = [pl.BlockSpec(memory_space=pltpu.VMEM)] * 10 + [pl.BlockSpec(memory_space=pl.ANY)] * 4
    return pl.pallas_call(
        kernel,
        out_shape=[jax.ShapeDtypeStruct((rows, hidden), f32)] * 2,
        in_specs=specs,
        out_specs=[pl.BlockSpec(memory_space=pltpu.VMEM)] * 2,
        scratch_shapes=scratch,
        compiler_params=pltpu.CompilerParams(
            collective_id=0, has_side_effects=True, vmem_limit_bytes=67043328
        ),
    )(*operands)


def fused_body(mesh):
    def run(
        latents, labels, step_index, seeds, class_table,
        teacher_patch, teacher_mod, teacher_up, teacher_down, teacher_out,
        student_patch, student_mod, student_up, student_down, student_out,
    ):
        samples = latents.shape[0]
        rows = teacher_up.shape[0]
        group = D // rows
        now = step_index.astype(jnp.float32) / STEPS
        times = jnp.stack([now, now - 0.5 / STEPS, now - 1.0 / STEPS])
        alphas, sigmas = plan(times)
        noisy = alphas[0][:, None, None] * latents + sigmas[0][:, None, None] * noise_of(seeds)
        lanes = noisy.reshape(samples, 2, TILE, PATCH).transpose(3, 1, 0, 2)
        lanes = lanes.reshape(PATCH, samples * SEQ)
        coef = jnp.stack(
            [alphas[0], sigmas[0], alphas[1], sigmas[1], alphas[2], sigmas[2], now, now]
        )
        coef = jnp.broadcast_to(coef[:, :, None], (8, samples, TILE)).reshape(8, samples * TILE)
        onehot = labels[:, None] == jnp.arange(CLASSES, dtype=jnp.int32)[None, :]
        embedded = jnp.dot(
            onehot.astype(jnp.bfloat16), class_table, preferred_element_type=jnp.float32
        )
        features = time_features(times[:2].reshape(-1))
        cond = jax.nn.silu(jnp.concatenate([embedded, embedded]) + features).astype(jnp.bfloat16)
        cond = jnp.pad(cond.astype(jnp.float32), ((0, 8 - 2 * samples), (0, 0)))
        cond = cond.reshape(8, group, rows).transpose(1, 0, 2)
        tabs = jnp.asarray(position_tables())
        operands = (
            lanes, coef, cond,
            teacher_mod.transpose(1, 0, 2), student_mod.transpose(1, 0, 2), tabs,
            teacher_patch, student_patch, teacher_out, student_out,
            teacher_up, teacher_down, student_up, student_down,
        )
        up_gradient, down_gradient = fused_call(mesh, operands)
        return up_gradient, down_gradient

    return run


def choose(mesh):
    sizes = dict(mesh.shape)
    fits = sizes["dp"] == 2 and sizes["row"] == 4 and sizes["col"] > 1
    return fused_body(mesh) if fits else body


def solution(mesh):
    placed = (
        P(("dp", "row"), None, None),
        P(("dp", "row")),
        P(("dp", "row")),
        P(("dp", "row")),
        P(),
        P(),
        P(("dp", "row"), None, "col"),
        P(("dp", "row"), "col"),
        P(("dp", "row"), "col"),
        P(),
        P(),
        P(("dp", "row"), None, "col"),
        P(("dp", "row"), "col"),
        P(("dp", "row"), "col"),
        P(),
    )
    return jax.shard_map(
        choose(mesh),
        mesh=mesh,
        in_specs=placed,
        out_specs=(P(("dp", "row"), "col"), P(("dp", "row"), "col")),
        check_vma=False,
    )
```

```python
import math

import jax
import jax.numpy as jnp
import numpy as np
from jax import lax
from jax.experimental import pallas as pl
from jax.experimental.pallas import tpu as pltpu
from jax.sharding import PartitionSpec as P

D = 1152
CLASSES = 1000
SEQ = 256
PATCH = 16
STEPS = 8


HALF_PI = 0.5 * math.pi
ROOT_TWO_PI = math.sqrt(2.0 / math.pi)


def plan(times):
    return (jnp.cos(HALF_PI * times), jnp.sin(HALF_PI * times))


def mixing(value):
    amount = jnp.int32(16)
    value = value ^ lax.shift_right_logical(value, amount)
    value = value * 73244475
    value = value ^ lax.shift_right_logical(value, amount)
    value = value * 73244475
    value = value ^ lax.shift_right_logical(value, amount)
    return value


def noise_of(seeds):
    total = SEQ * PATCH
    places = jnp.arange(total, dtype=jnp.int32).reshape(1, total // 128, 128)
    mixed = mixing(seeds[:, None, None] * 1103515245 + places * 40503 + 12345)
    uniform = (lax.shift_right_logical(mixed, jnp.int32(8)).astype(jnp.float32) + 0.5) * (
        1.0 / 16777216.0
    )
    return math.sqrt(2.0) * lax.erf_inv(2.0 * uniform - 1.0)


def time_features(times):
    half = D // 2
    freqs = jnp.exp(-math.log(10000.0) * jnp.arange(half, dtype=jnp.float32) / half)
    angle = (1000.0 * times)[:, None] * freqs[None, :]
    return jnp.concatenate([jnp.cos(angle), jnp.sin(angle)], axis=1)


def condition(times, labels, class_table):
    onehot = (labels[:, None] == jnp.arange(CLASSES, dtype=jnp.int32)[None, :]).astype(jnp.bfloat16)
    embedded = jnp.dot(onehot, class_table, preferred_element_type=jnp.float32)
    return jax.nn.silu(embedded + time_features(times)).astype(jnp.bfloat16)


def positions():
    quarter = D // 4
    omega = 1.0 / 10000.0 ** (jnp.arange(quarter, dtype=jnp.float32) / quarter)
    side = math.isqrt(SEQ)
    cells = jnp.arange(SEQ, dtype=jnp.int32)
    grid_row = (cells // side).astype(jnp.float32)
    grid_col = (cells % side).astype(jnp.float32)
    row_angle = grid_row[:, None] * omega[None, :]
    col_angle = grid_col[:, None] * omega[None, :]
    return jnp.concatenate(
        [jnp.sin(row_angle), jnp.cos(row_angle), jnp.sin(col_angle), jnp.cos(col_angle)], axis=1
    )


def layer_norm(values):
    center = values - jnp.mean(values, axis=-1, keepdims=True)
    spread = jnp.mean(center * center, axis=-1, keepdims=True)
    reciprocal = lax.rsqrt(spread + 1e-06)
    return (center * reciprocal, reciprocal)


def gelu_slope(pre):
    inner = ROOT_TWO_PI * (pre + 0.044715 * pre * pre * pre)
    tangent = jnp.tanh(inner)
    return 0.5 * (1.0 + tangent) + 0.5 * pre * (1.0 - tangent * tangent) * ROOT_TWO_PI * (
        1.0 + 3.0 * 0.044715 * pre * pre
    )


def contract_last(left, right):
    return lax.dot_general(
        left, right, (((1,), (1,)), ((), ())), preferred_element_type=jnp.float32
    )


def contract_first(left, right):
    return lax.dot_general(
        left, right, (((0,), (0,)), ((), ())), preferred_element_type=jnp.float32
    )


def modulate(base, mods):
    normed, _ = layer_norm(base)
    shift = mods[0][None, :, None, :]
    scale = mods[1][None, :, None, :]
    return (normed * (1.0 + scale) + shift).astype(jnp.bfloat16).reshape(-1, D)


def embed(tokens, patch_weight, pos):
    flat = tokens.reshape(-1, PATCH)
    product = jnp.dot(flat, patch_weight, preferred_element_type=jnp.float32)
    return product.reshape(*tokens.shape[:-1], D) + pos


def scatter_columns(partial_out, groups):
    blocks = partial_out.reshape(groups, -1, D)
    swapped = lax.all_to_all(blocks, "col", split_axis=0, concat_axis=0, tiled=True)
    return jnp.sum(swapped.astype(jnp.float32), axis=0)


def reduce_gradient(left, right, group):
    names = ("dp", "row")
    me = lax.axis_index(names)
    pairs = group // 2
    mine, parity = me // 2, me % 2
    partial = contract_first(left, right)
    blocks = partial.reshape(pairs, 2, partial.shape[0] // group, partial.shape[1])
    keep = lax.dynamic_index_in_dim(blocks, parity, 1, keepdims=False)
    give = lax.dynamic_index_in_dim(blocks.astype(jnp.bfloat16), 1 - parity, 1, keepdims=False)
    got = lax.ppermute(give, names, [(i, i ^ 1) for i in range(group)])
    pair = keep + got.astype(jnp.float32)
    sent = pair.astype(jnp.bfloat16)
    total = lax.dynamic_index_in_dim(pair, mine, 0, keepdims=False)
    for step in range(1, pairs):
        piece = lax.dynamic_index_in_dim(sent, (mine + step) % pairs, 0, keepdims=False)
        hop = [(i, (i + 2 * step) % group) for i in range(group)]
        total = total + lax.ppermute(piece, names, hop).astype(jnp.float32)
    return total


def body(
    latents,
    labels,
    step_index,
    seeds,
    class_table,
    teacher_patch,
    teacher_mod,
    teacher_up,
    teacher_down,
    teacher_out,
    student_patch,
    student_mod,
    student_up,
    student_down,
    student_out,
):
    samples = latents.shape[0]
    group = lax.axis_size(("dp", "row"))
    groups = lax.axis_size("col")
    column = lax.axis_index("col")
    chunk = SEQ // groups
    batch_total = samples * group
    up_panel, down_panel, student_up_panel, student_panel = [
        lax.all_gather(weight, ("dp", "row"), axis=0, tiled=True)
        for weight in (teacher_up, teacher_down, student_up, student_down)
    ]
    both = lax.all_gather(jnp.stack([labels, step_index]), ("dp", "row"), axis=1, tiled=True)
    all_labels, all_steps = both[0], both[1]
    all_now = all_steps.astype(jnp.float32) / STEPS
    cond = condition(
        jnp.concatenate([all_now, all_now - 0.5 / STEPS]),
        jnp.concatenate([all_labels, all_labels]),
        class_table,
    )
    own_rows = teacher_mod.shape[0]
    offset = lax.axis_index(("dp", "row")) * own_rows
    rows = lax.dynamic_slice_in_dim(cond, offset, own_rows, 1)
    width = teacher_mod.shape[2]
    parts = []
    for taken, weights in ((2, teacher_mod), (1, student_mod)):
        for index in range(3):
            product = jnp.dot(
                rows[: taken * batch_total],
                weights[:, index],
                preferred_element_type=jnp.float32,
            ).reshape(taken, group, samples, width)
            parts.extend(product[which] for which in range(taken))
    parts = jnp.concatenate(parts, axis=1)
    swapped = lax.all_to_all(parts, ("dp", "row"), split_axis=0, concat_axis=0, tiled=True)
    sums = jnp.sum(swapped, axis=0)
    gathered = lax.all_gather(sums, "col", axis=0, tiled=False)
    joined = jnp.concatenate([gathered[place] for place in range(groups)], axis=-1)

    def entry(place):
        return joined[place * samples : (place + 1) * samples]

    teacher_now = [entry(2 * index) for index in range(3)]
    teacher_mid = [entry(2 * index + 1) for index in range(3)]
    student_mods = [entry(6 + index) for index in range(3)]

    now = step_index.astype(jnp.float32) / STEPS
    alpha, sigma = plan(now[:, None, None])
    alpha_mid, sigma_mid = plan((now - 0.5 / STEPS)[:, None, None])
    alpha_end, sigma_end = plan((now - 1.0 / STEPS)[:, None, None])
    noisy_full = alpha * latents + sigma * noise_of(seeds)
    noisy_full = noisy_full.reshape(samples, groups, chunk, PATCH).transpose(1, 0, 2, 3)
    noisy = lax.dynamic_index_in_dim(noisy_full, column, 0, keepdims=False)
    noisy_tokens = noisy_full.astype(jnp.bfloat16)
    pos = positions().reshape(groups, 1, chunk, D)
    own_pos = lax.dynamic_index_in_dim(pos, column, 0, keepdims=True)

    def own_output(own_base, gate, mixed, out_weight):
        later = own_base[0] + gate[:, None, :] * mixed.reshape(samples, chunk, D)
        final, _ = layer_norm(later)
        velocity = contract_last(final.astype(jnp.bfloat16).reshape(-1, D), out_weight)
        return velocity.reshape(samples, chunk, PATCH)

    def teacher(tokens, own_tokens, these):
        act = modulate(embed(tokens, teacher_patch, pos), these)
        pre = jnp.dot(act, up_panel, preferred_element_type=jnp.float32)
        hidden = jax.nn.gelu(pre, approximate=True).astype(jnp.bfloat16)
        mixed = scatter_columns(contract_last(hidden, down_panel).astype(jnp.bfloat16), groups)
        own_base = embed(own_tokens[None], teacher_patch, own_pos)
        return own_output(own_base, these[2], mixed, teacher_out)

    first_v = teacher(noisy_tokens, noisy.astype(jnp.bfloat16), teacher_now)
    first_x = alpha * noisy - sigma * first_v
    halfway = alpha_mid * first_x + sigma_mid * (noisy - alpha * first_x) / sigma
    halfway_own = halfway.astype(jnp.bfloat16)
    halfway_tokens = lax.all_gather(halfway_own, "col", axis=0, tiled=False)
    gate = student_mods[2]
    base = embed(noisy_tokens, student_patch, pos)
    act = modulate(base, student_mods)
    pre = jnp.dot(act, student_up_panel, preferred_element_type=jnp.float32)
    hidden = jax.nn.gelu(pre, approximate=True).astype(jnp.bfloat16)
    hidden, halfway_tokens = lax.optimization_barrier((hidden, halfway_tokens))
    second_v = teacher(halfway_tokens, halfway_own, teacher_mid)
    second_x = alpha_mid * halfway - sigma_mid * second_v
    landing = alpha_end * second_x + sigma_end * (halfway - alpha_mid * second_x) / sigma_mid
    ratio = sigma_end / sigma
    target = (landing - ratio * noisy) / (alpha_end - ratio * alpha)

    own_mixed = scatter_columns(contract_last(hidden, student_panel).astype(jnp.bfloat16), groups)
    own_base = embed(noisy.astype(jnp.bfloat16)[None], student_patch, own_pos)[0]
    later = own_base + gate[:, None, :] * own_mixed.reshape(samples, chunk, D)
    final, reciprocal = layer_norm(later)
    student_v = contract_last(final.astype(jnp.bfloat16).reshape(-1, D), student_out)
    student_x = alpha * noisy - sigma * student_v.reshape(samples, chunk, PATCH)
    weight = jnp.maximum(alpha * alpha / (sigma * sigma), 1.0)
    back_velocity = -2.0 * sigma * weight * (student_x - target) / batch_total
    back_final = jnp.dot(
        back_velocity.reshape(-1, PATCH),
        student_out.astype(jnp.float32),
        precision=lax.Precision.HIGHEST,
    ).reshape(samples, chunk, D)
    centre = jnp.mean(back_final, axis=2, keepdims=True)
    along = jnp.mean(back_final * final, axis=2, keepdims=True)
    own_back = (
        gate[:, None, :] * (reciprocal * (back_final - centre - final * along))
    ).astype(jnp.bfloat16)
    back_mixed = lax.all_gather(own_back.reshape(-1, D), "col", axis=0, tiled=True)
    back_hidden = jnp.dot(back_mixed, student_panel, preferred_element_type=jnp.float32)
    back_pre = (back_hidden * gelu_slope(pre)).astype(jnp.bfloat16)
    down_gradient = reduce_gradient(back_mixed, hidden, group)
    up_gradient = reduce_gradient(act, back_pre, group)
    return (up_gradient, down_gradient)


TILE = 128
BLOCK = 384
MESH = pl.DeviceIdType.MESH


def ln_parts(values):
    center = values - jnp.mean(values, axis=-1, keepdims=True)
    spread = jnp.mean(center * center, axis=-1, keepdims=True)
    reciprocal = lax.rsqrt(spread + 1e-06)
    return center * reciprocal, reciprocal


def position_tables():
    quarter = D // 4
    side = math.isqrt(SEQ)
    omega = 1.0 / 10000.0 ** (np.arange(quarter, dtype=np.float32) / np.float32(quarter))
    angle = np.arange(side, dtype=np.float32)[:, None] * omega[None, :].astype(np.float32)
    table = np.concatenate([np.sin(angle), np.cos(angle)], axis=1).astype(np.float32)
    blank = np.zeros_like(table)
    return np.stack(
        [np.concatenate([table, blank], axis=1), np.concatenate([blank, table], axis=1)]
    )


def feature_table():
    half = D // 2
    freqs = np.exp(-math.log(10000.0) * np.arange(half, dtype=np.float64) / half)
    return np.tile(np.concatenate([freqs, freqs])[None, :], (8, 1)).astype(np.float32)


def fused_kernel(sizes, *refs):
    ring, line, samples, rows = sizes
    (labels, steps_in, seeds, lat, tabs, freq, pt, ps, ot, os_) = refs[:10]
    (table_in, tmod_in, smod_in, tup, tdn, sup, sdn) = refs[10:17]
    ug, dg = refs[17:19]
    (
        table, tmod, smod, wtu, wtd, wsu, wsd, nz, coef, cond, condall, mpart, mrecv, msum, modb,
        actt, acts, hidt, hids, pres, part, recv, mixed, recip, half, student,
        back, full, ugrad, dgrad, pairu, paird, sendu, sendd, crossu, crossd,
        loc, ws, wr, cs, cr, ms, mr, zs, zr, ls, lr, hs, hr, bs, br, gps, gpr, gcs, gcr,
    ) = refs[19:]
    bpre = hidt
    chips = 4
    group = 2 * chips
    blocks = D // BLOCK
    chunks = samples * blocks
    far = line - 1
    scope = jax.named_scope
    dp, row, col = lax.axis_index("dp"), lax.axis_index("row"), lax.axis_index("col")
    me = dp * ring + row
    chip, core = me // 2, me % 2
    sib = me + 1 - 2 * core
    over_x = (1 - dp) * ring + row
    over_y = dp * ring + (row + 2) % ring
    over_xy = (1 - dp) * ring + (row + 2) % ring
    owner = (col == 0) | (col == far)
    mine = col // far

    def member(index):
        return {"dp": index // ring, "row": index % ring}

    def sibling(index):
        return index + 1 - 2 * (index % 2)

    def chip_at(offset):
        return (chip + offset) % chips

    def remote(src, dst, send, recv_sem, where):
        return pltpu.make_async_remote_copy(
            src_ref=src, dst_ref=dst, send_sem=send, recv_sem=recv_sem,
            device_id=where, device_id_type=MESH,
        )

    def loop(count, step):
        def run(i, carry):
            step(i)
            return carry

        lax.fori_loop(0, count, run, 0)

    def aligned(start, size, unit):
        return pl.ds(pl.multiple_of(start, unit), size)

    barrier = pltpu.get_barrier_semaphore()
    for offset in range(1, group):
        pl.semaphore_signal(barrier, inc=1, device_id=member((me + offset) % group), device_id_type=MESH)
    for offset in range(1, line):
        pl.semaphore_signal(barrier, inc=1, device_id={"col": (col + offset) % line}, device_id_type=MESH)

    panels = (wtu, wtd, wsu, wsd)
    top = (rows // 2 + 15) // 16 * 16

    def slot(w, index):
        return panels[w].at[aligned(index * rows, rows, 16), :]

    def upper(w, index):
        return panels[w].at[aligned(index * rows, top, 16), :]

    def lower(w, index):
        return panels[w].at[aligned(index * rows + top, rows - top, 16), :]

    fetches = [pltpu.make_async_copy(table_in, table, loc.at[0])]
    for w, shard in enumerate((tup, tdn, sup, sdn)):
        fetches.append(pltpu.make_async_copy(shard, slot(w, me), loc.at[1 + w]))
    fetches.append(pltpu.make_async_copy(tmod_in, tmod, loc.at[5]))
    fetches.append(pltpu.make_async_copy(smod_in, smod, loc.at[6]))
    for order in (0, 1, 5, 2, 6, 3, 4):
        fetches[order].start()

    def moves(w):
        return [
            (upper, me, over_y), (lower, me, over_x), (lower, me, over_y), (upper, me, over_x),
            (upper, over_y, over_x), (lower, over_x, over_y),
            (slot, me, sib), (slot, over_x, sib), (slot, over_y, sib), (slot, over_xy, sib),
        ]

    def landings(w):
        return [
            (upper, over_y, over_y), (lower, over_x, over_x), (lower, over_y, over_y), (upper, over_x, over_x),
            (upper, over_xy, over_x), (lower, over_xy, over_y),
            (slot, sib, sib), (slot, sibling(over_x), sib), (slot, sibling(over_y), sib),
            (slot, sibling(over_xy), sib),
        ]

    def weight_copy(entries, w, index):
        view, place, where = entries[index]
        ref = view(w, place)
        return remote(ref, ref, ws.at[w, index], wr.at[w, index], member(where))

    def send(w, index):
        return weight_copy(moves(w), w, index)

    def arrival(w, index):
        return weight_copy(landings(w), w, index)

    def own_send(w):
        for index in range(4):
            send(w, index).start()
        send(w, 6).start()

    def relay(w):
        for index in (0, 1):
            arrival(w, index).wait_recv()
            send(w, 4 + index).start()

    def pass_near(w):
        arrival(w, 3).wait_recv()
        send(w, 7).start()
        arrival(w, 2).wait_recv()
        send(w, 8).start()

    def pass_far(w):
        arrival(w, 4).wait_recv()
        arrival(w, 5).wait_recv()
        send(w, 9).start()

    def collect(w):
        for index in range(6, 10):
            arrival(w, index).wait_recv()

    def cond_copy(offset):
        return remote(cond.at[(me + offset) % group], condall.at[me], cs.at[offset - 1], cr.at[offset - 1],
                      member((me + offset) % group))

    spans = ((0, 2), (2, 4))

    def mod_copy(stage, offset):
        piece = pl.ds(*spans[stage])
        return remote(mpart.at[(me + offset) % group, piece], mrecv.at[offset - 1, piece],
                      ms.at[stage, offset - 1], mr.at[stage, offset - 1], member((me + offset) % group))

    def line_copy(stage, offset):
        piece = pl.ds(*spans[stage])
        return remote(msum.at[col, piece], msum.at[col, piece], zs.at[stage, offset - 1], zr.at[stage, offset - 1],
                      {"col": (col + offset) % line})

    def mods_start(stage):
        for offset in range(1, group):
            mod_copy(stage, offset).start()

    def mods_sum(stage):
        piece = pl.ds(*spans[stage])
        total = mpart[me, piece]
        for offset in range(1, group):
            mod_copy(stage, offset).wait_recv()
            total = total + mrecv[offset - 1, piece]
        msum[col, piece] = total
        for offset in range(1, line):
            line_copy(stage, offset).start()

    def mods_join(stage):
        width = msum.shape[3]
        for offset in range(1, line):
            line_copy(stage, offset).wait_recv()
        first, count = spans[stage]
        for place in range(line):
            for entry in range(first, first + count):
                modb[entry, :, place * width : (place + 1) * width] = msum[place, entry]

    def times_of(s):
        return steps_in[s].astype(jnp.float32) / STEPS

    def schedule():
        kind = lax.broadcasted_iota(jnp.int32, (8, TILE), 0)
        back_by = (kind // 2).astype(jnp.float32) * (0.5 / STEPS)
        for s in range(samples):
            angle = HALF_PI * (times_of(s) - back_by)
            coef[:, s * TILE : (s + 1) * TILE] = jnp.where(kind % 2 == 0, jnp.cos(angle), jnp.sin(angle))

    def conditioning():
        count = 16
        line_of = lax.broadcasted_iota(jnp.int32, (count, CLASSES), 0)
        lane_of = lax.broadcasted_iota(jnp.int32, (count, CLASSES), 1)
        wanted = jnp.full((count, CLASSES), -1, jnp.int32)
        kind = lax.broadcasted_iota(jnp.int32, (8, D), 0)
        time = jnp.zeros((8, D), jnp.float32)
        for s in range(samples):
            for late in range(2):
                place = late * samples + s
                wanted = jnp.where(line_of == place, labels[s], wanted)
                time = jnp.where(kind == place, times_of(s) - late * (0.5 / STEPS), time)
        onehot = jnp.where(wanted == lane_of, 1.0, 0.0).astype(jnp.bfloat16)
        angle = (1000.0 * time) * freq[...]
        lane = lax.broadcasted_iota(jnp.int32, (8, D), 1)
        features = jnp.where(lane < D // 2, jnp.cos(angle), jnp.sin(angle))
        fetches[0].wait()
        embedded = jnp.dot(onehot, table[...], preferred_element_type=jnp.float32)[:8]
        value = embedded + features
        value = (value * jax.nn.sigmoid(value)).astype(jnp.bfloat16).astype(jnp.float32)
        for j in range(group):
            cond[j] = value[:, j * rows : (j + 1) * rows]

    def noise():
        place = lax.broadcasted_iota(jnp.int32, (PATCH, SEQ), 1) * PATCH
        place = place + lax.broadcasted_iota(jnp.int32, (PATCH, SEQ), 0)
        for s in range(samples):
            mixed_bits = mixing(seeds[s] * jnp.int32(1103515245) + place * 40503 + 12345)
            uniform = (lax.shift_right_logical(mixed_bits, jnp.int32(8)).astype(jnp.float32) + 0.5) * (
                1.0 / 16777216.0
            )
            drawn = math.sqrt(2.0) * lax.erf_inv(2.0 * uniform - 1.0)
            alpha = coef[0:1, s * TILE : s * TILE + 1]
            sigma = coef[1:2, s * TILE : s * TILE + 1]
            where = slice(s * SEQ, (s + 1) * SEQ)
            nz[:, where] = alpha * lat[:, where] + sigma * drawn

    with scope("barrier"):
        schedule()
        pl.semaphore_wait(barrier, group - 1 + line - 1)
    with scope("first"):
        fetches[1].wait()
        send(0, 0).start()
        send(0, 1).start()
    with scope("cond"):
        conditioning()
        for offset in range(1, group):
            cond_copy(offset).start()
        for index in (2, 3, 6):
            send(0, index).start()
    with scope("noise"):
        condall[me] = cond[me]
        noise()
        fetches[5].wait()
        fetches[6].wait()
    with scope("cond_wait"):
        for offset in range(1, group):
            cond_copy(offset).wait_recv()
    with scope("mod_part"):
        lhs = condall[...].reshape(group * 8, rows).astype(jnp.bfloat16)

        def project(entry):
            weights = (tmod if entry < 3 else smod)[entry % 3]
            product = jnp.dot(lhs, weights, preferred_element_type=jnp.float32)
            mpart[:, entry] = product.reshape(group, 8, product.shape[1])

        project(0)
        project(1)
        mods_start(0)
        for entry in range(2, 6):
            project(entry)
    with scope("relay0"):
        relay(0)
        for order in (2, 3, 4):
            fetches[order].wait()
        own_send(1)
        pass_near(0)
    with scope("mod_sum"):
        mods_sum(0)
    with scope("far0"):
        pass_far(0)
    with scope("mod_join"):
        mods_join(0)

    def tokens(index):
        return aligned(index * TILE, TILE, TILE)

    def rows_of(s):
        return aligned(s * SEQ, SEQ, SEQ)

    def place_of(h):
        side = SEQ // 16
        rows_in = tabs[0, aligned(h * 8, 8, 8), :]
        grid = jnp.broadcast_to(rows_in[:, None, :], (8, side, D)) + tabs[1][None]
        return grid.reshape(TILE, D)

    def base_of(state, patch, h):
        flat = state.T.astype(jnp.bfloat16)
        return jnp.dot(flat, patch[...], preferred_element_type=jnp.float32) + place_of(h)

    def noisy_of(h, s):
        return nz[:, tokens(2 * s + h)]

    def half_of(h, s):
        return half[h, :, tokens(s)]

    def act_tiles(s, state, patch, first, shift_row, out, start):
        def step(h):
            normed, _ = ln_parts(base_of(state(h, s), patch, h))
            shift = modb[first, pl.ds(shift_row + s, 1), :]
            scale = modb[first + 1, pl.ds(shift_row + s, 1), :]
            out[aligned(start + h * TILE, TILE, TILE), :] = (normed * (1.0 + scale) + shift).astype(jnp.bfloat16)

        loop(2, step)

    def up_tile(s, act, start, panel, hidden, keep):
        pre = jnp.dot(act[aligned(start, SEQ, SEQ), :], panel[...], preferred_element_type=jnp.float32)
        if keep is not None:
            keep[rows_of(s), :] = pre
        hidden[rows_of(s), :] = jax.nn.gelu(pre, approximate=True).astype(jnp.bfloat16)

    def hop_of(h):
        return h * col + (1 - h) * (far - col)

    def chunk_copy(h, c):
        return remote(part.at[h, c], recv.at[h, c], ls.at[h, c], lr.at[h, c], {"col": col + 2 * h - 1})

    def down_tile(s, hidden, panel, first, reuse):
        if reuse:
            for h in (1, 0):
                @pl.when(hop_of(h) < far)
                def _():
                    for f in range(blocks):
                        chunk_copy(h, first + s * blocks + f).wait_send()
        product = contract_last(hidden[rows_of(s), :], panel[...]).astype(jnp.bfloat16)
        for h in (1, 0):
            for f in range(blocks):
                part[h, first + s * blocks + f] = product[h * TILE : (h + 1) * TILE, f * BLOCK : (f + 1) * BLOCK]

    def back_copy(h, j):
        return remote(back.at[h, j], back.at[h, j], bs.at[h, j], br.at[h, j], {"col": col + 1 - 2 * h})

    fill = 2 * far
    student_at = chunks + 1
    second_at = student_at + chunks
    back_at = second_at + blocks + fill

    def steps(start, stop):
        def step(t, carry):
            for h in (1, 0):
                hop = hop_of(h)
                n = t - 2 * hop + jnp.where(hop == 0, 1, 0)
                early = jnp.where(n < chunks, 1, 0)
                late = jnp.where(n >= second_at, 1, 0)
                c = early * n + late * (n - second_at) + (1 - early - late) * (n - student_at + chunks)
                inside = (n >= 0) & (n < second_at + chunks) & ((n < chunks) | (n >= student_at))

                @pl.when(inside & (hop == 0))
                def _():
                    chunk_copy(h, c).start()

                @pl.when(inside & (hop > 0))
                def _():
                    chunk_copy(h, c).wait_recv()
                    sum_ = part[h, c].astype(jnp.float32) + recv[h, c].astype(jnp.float32)

                    @pl.when(hop < far)
                    def _():
                        part[h, c] = sum_.astype(jnp.bfloat16)
                        chunk_copy(h, c).start()

                    @pl.when(hop == far)
                    def _():
                        mixed[c] = sum_

            return carry

        lax.fori_loop(start, stop, step, 0)

    def back_steps(start, stop):
        def step(t, carry):
            for h in (0, 1):
                hop = far - hop_of(h)
                j = t - back_at - 2 * hop

                @pl.when((hop > 0) & (j >= 0) & (j < chunks))
                def _():
                    back_copy(h, j).wait_recv()

                    @pl.when(hop < far)
                    def _():
                        back_copy(h, j).start()

                    where = aligned((j // blocks) * SEQ + h * TILE, TILE, TILE)
                    full[where, aligned((j % blocks) * BLOCK, BLOCK, BLOCK)] = back[h, j]

            return carry

        lax.fori_loop(start, stop, step, 0)

    def later_of(state, patch, first, s, gate):
        sums = [mixed[first + s * blocks + f] for f in range(blocks)]
        return base_of(state, patch, mine) + gate * jnp.concatenate(sums, axis=1)

    def velocity_of(final, out):
        return contract_last(out[...], final.astype(jnp.bfloat16))

    def row_of(index, s):
        return coef[index : index + 1, tokens(s)]

    def half_copy(s, offset):
        piece = half.at[mine, :, tokens(s)]
        return remote(piece, piece, hs.at[s, offset - 1], hr.at[mine, s, offset - 1],
                      {"col": (col + offset) % line})

    def first_stage(s):
        @pl.when(owner)
        def _():
            noisy = noisy_of(mine, s)
            final, _ = ln_parts(later_of(noisy, pt, 0, s, modb[2, pl.ds(s, 1), :]))
            speed = velocity_of(final, ot)
            alpha, sigma, alpha_mid, sigma_mid = [row_of(index, s) for index in range(4)]
            first_x = alpha * noisy - sigma * speed
            half[mine, :, tokens(s)] = alpha_mid * first_x + sigma_mid * (noisy - alpha * first_x) / sigma
            for offset in range(1, line):
                half_copy(s, offset).start()

    def half_wait(s):
        for h in range(2):
            source = h * far
            for offset in range(1, line):
                @pl.when((source + offset) % line == col)
                def _():
                    piece = half.at[h, :, tokens(s)]
                    remote(piece, piece, hs.at[s, offset - 1], hr.at[h, s, offset - 1], {"col": source}).wait_recv()

    def student_stage(s):
        @pl.when(owner)
        def _():
            noisy = noisy_of(mine, s)
            final, reciprocal = ln_parts(later_of(noisy, ps, chunks, s, modb[5, pl.ds(s, 1), :]))
            speed = velocity_of(final, os_)
            student[:, tokens(s)] = row_of(0, s) * noisy - row_of(1, s) * speed
            recip[s] = jnp.broadcast_to(reciprocal, (TILE, TILE))
            for f in range(blocks):
                mixed[chunks + s * blocks + f] = final[:, f * BLOCK : (f + 1) * BLOCK]

    def back_stage(s):
        @pl.when(owner)
        def _():
            noisy, middle = noisy_of(mine, s), half_of(mine, s)
            reached, _ = ln_parts(later_of(middle, pt, 0, s, modb[2, pl.ds(samples + s, 1), :]))
            speed = velocity_of(reached, ot)
            alpha, sigma, alpha_mid, sigma_mid, alpha_end, sigma_end = [row_of(index, s) for index in range(6)]
            second_x = alpha_mid * middle - sigma_mid * speed
            landing = alpha_end * second_x + sigma_end * (middle - alpha_mid * second_x) / sigma_mid
            ratio = sigma_end / sigma
            target = (landing - ratio * noisy) / (alpha_end - ratio * alpha)
            weight = jnp.maximum(alpha * alpha / (sigma * sigma), 1.0)
            speed_back = -2.0 * sigma * weight * (student[:, tokens(s)] - target) / (samples * group)
            high = speed_back.astype(jnp.bfloat16).astype(jnp.float32)
            rest = speed_back - high
            medium = rest.astype(jnp.bfloat16).astype(jnp.float32)
            low = rest - medium
            pieces = jnp.concatenate([high, medium, low], axis=0).T.astype(jnp.bfloat16)
            outs = jnp.concatenate([os_[...]] * 3, axis=0)
            back_final = jnp.dot(pieces, outs, preferred_element_type=jnp.float32)
            final = jnp.concatenate([mixed[chunks + s * blocks + f] for f in range(blocks)], axis=1)
            gate = modb[5, pl.ds(s, 1), :]
            centre = jnp.mean(back_final, axis=-1, keepdims=True)
            along = jnp.mean(back_final * final, axis=-1, keepdims=True)
            own = (gate * (recip[s, :, 0:1] * (back_final - centre - final * along))).astype(jnp.bfloat16)
            for f in range(blocks):
                back[mine, s * blocks + f] = own[:, f * BLOCK : (f + 1) * BLOCK]
                back_copy(mine, s * blocks + f).start()
            full[aligned(s * SEQ + mine * TILE, TILE, TILE), :] = own

    def outer(s, left, right, grad):
        def step(r):
            where = aligned(r * BLOCK, BLOCK, BLOCK)
            value = contract_first(left[rows_of(s), where], right[rows_of(s), :])
            grad[where, :] = grad[where, :] + value

        loop(blocks, step)

    def back_pre(s):
        hidden_back = jnp.dot(full[rows_of(s), :], wsd[...], preferred_element_type=jnp.float32)
        bpre[rows_of(s), :] = (hidden_back * gelu_slope(pres[rows_of(s), :])).astype(jnp.bfloat16)

    def teacher_up(s, state, shift_row):
        act_tiles(s, state, pt, 0, shift_row, actt, 0)
        up_tile(s, actt, 0, wtu, hidt, None)

    with scope("t1_a"):
        act_tiles(0, noisy_of, pt, 0, 0, actt, 0)
        relay(1)
        mods_start(1)
        own_send(2)
    with scope("collect0"):
        collect(0)
    with scope("t1_b"):
        up_tile(0, actt, 0, wtu, hidt, None)
        pass_near(1)

        def rest(i):
            teacher_up(i + 1, noisy_of, 0)

            @pl.when(i == 0)
            def _():
                pass_far(1)

        loop(samples - 1, rest)
    with scope("collect1"):
        collect(1)
    with scope("t1_down"):
        down_tile(0, hidt, wtd, 0, False)
        steps(-1, 0)
        loop(samples - 1, lambda i: down_tile(i + 1, hidt, wtd, 0, False))

    events = {}

    def at(t, name, *calls):
        events.setdefault(t, []).append((name, calls))

    def student_up(s):
        up_tile(s, acts, s * SEQ, wsu, hids, pres)

    def clear():
        dgrad[...] = jnp.zeros_like(dgrad)
        ugrad[...] = jnp.zeros_like(ugrad)

    at(0, "mods1", lambda: mods_sum(1))
    at(1, "relay2", lambda: relay(2), lambda: own_send(3))
    at(3, "join1", lambda: mods_join(1))
    for s in range(samples):
        at(3 + s, "s_act%d" % s, lambda s=s: act_tiles(s, noisy_of, ps, 3, 0, acts, s * SEQ))
    at(4, "near2", lambda: pass_near(2))
    at(6, "far2", lambda: pass_far(2), lambda: relay(3), lambda: collect(2))
    for s in range(samples):
        at(7 + s, "s_up%d" % s, lambda s=s: student_up(s))
    at(8, "near3", lambda: pass_near(3))
    at(9, "far3", lambda: pass_far(3), lambda: collect(3))
    for s in range(samples):
        ready = blocks * (s + 1) + fill
        at(ready, "own%d" % s, lambda s=s: first_stage(s))
        at(ready + 2, "half%d" % s, lambda s=s: half_wait(s))
        at(ready + 2, "t2_%d" % s, lambda s=s: teacher_up(s, half_of, samples))
        at(student_at - 1 + blocks * s, "s_down%d" % s, lambda s=s: down_tile(s, hids, wsd, chunks, False))
        at(second_at - 2 + blocks * s, "t2_down%d" % s, lambda s=s: down_tile(s, hidt, wtd, 0, True))
        at(student_at + blocks * (s + 1) + fill, "student%d" % s, lambda s=s: student_stage(s))
        at(back_at + blocks * s, "back%d" % s, lambda s=s: back_stage(s))
    at(second_at + 5, "clear", clear)

    finish_at = second_at + chunks + fill
    marks = sorted(set(events) | {0, back_at, finish_at})
    for place, t in enumerate(marks):
        for name, calls in events.get(t, []):
            with scope(name):
                for call in calls:
                    call()
        if t == finish_at:
            break
        until = marks[place + 1]
        with scope("line%d_%d" % (t, until)):
            if t < back_at:
                steps(t, until)
            else:
                def both(t_, carry):
                    steps(t_, t_ + 1)
                    back_steps(t_, t_ + 1)
                    return carry

                lax.fori_loop(t, until, both, 0)

    def pair_copy(grad, landing, which, offset):
        block = 2 * chip_at(offset) + 1 - core
        source = grad.at[aligned(block * rows, rows, 8), :]
        return remote(source, landing.at[offset], gps.at[which, offset], gpr.at[which, offset], member(sib))

    def pair_start(grad, landing, which):
        for offset in (2, 1, 3, 0):
            pair_copy(grad, landing, which, offset).start()

    upper_rows, lower_rows = pl.ds(0, top), pl.ds(top, rows - top)
    routes = (
        (0, upper_rows, over_x, 0), (0, lower_rows, over_y, 0),
        (1, upper_rows, over_x, 1), (2, lower_rows, over_y, 1),
        (2, upper_rows, over_y, 2), (1, lower_rows, over_x, 2),
    )

    def grad_copy(staged, landing, which, index):
        block, piece, where, _ = routes[index]
        target_block = (1, 1, 0, 0, 2, 2)[index]
        return remote(staged.at[block, piece], landing.at[target_block, piece], gcs.at[which, index],
                      gcr.at[which, index], member(where))

    def summed(grad, landing, place):
        block = place // 2
        offset = (block + chips - chip) % chips
        return grad[aligned(place * rows, rows, 8), :] + landing[offset]

    def cross_start(grad, landing, staged, received, which):
        for offset in (2, 1, 3, 0):
            pair_copy(grad, landing, which, offset).wait_recv()
        staged[0] = summed(grad, landing, over_xy).astype(jnp.bfloat16)
        grad_copy(staged, received, which, 0).start()
        grad_copy(staged, received, which, 1).start()
        staged[1, upper_rows] = summed(grad, landing, over_x)[:top].astype(jnp.bfloat16)
        grad_copy(staged, received, which, 2).start()
        staged[2, lower_rows] = summed(grad, landing, over_y)[top:].astype(jnp.bfloat16)
        grad_copy(staged, received, which, 3).start()

    def cross_next(grad, landing, staged, received, which):
        grad_copy(staged, received, which, 0).wait_recv()
        near_y = summed(grad, landing, over_y)[:top] + received[1, upper_rows].astype(jnp.float32)
        staged[2, upper_rows] = near_y.astype(jnp.bfloat16)
        grad_copy(staged, received, which, 4).start()
        grad_copy(staged, received, which, 1).wait_recv()
        near_x = summed(grad, landing, over_x)[top:] + received[1, lower_rows].astype(jnp.float32)
        staged[1, lower_rows] = near_x.astype(jnp.bfloat16)
        grad_copy(staged, received, which, 5).start()

    def finish(grad, landing, staged, received, which, out):
        for index in (2, 3):
            grad_copy(staged, received, which, index).wait_recv()
        sum_ = summed(grad, landing, me) + received[0].astype(jnp.float32)
        for index in (4, 5):
            grad_copy(staged, received, which, index).wait_recv()
        out[...] = sum_ + received[2].astype(jnp.float32)
        for index in range(6):
            grad_copy(staged, received, which, index).wait_send()
        for offset in range(chips):
            pair_copy(grad, landing, which, offset).wait_send()

    def gradient(s):
        with scope("relay"):
            back_steps(jnp.maximum(finish_at, back_at + fill + blocks * s), back_at + fill + blocks * (s + 1))
        with scope("dgrad"):
            outer(s, full, hids, dgrad)

        @pl.when(s == samples - 1)
        def _():
            pair_start(dgrad, paird, 0)

        with scope("bpre"):
            back_pre(s)

        @pl.when(s == samples - 1)
        def _():
            cross_start(dgrad, paird, sendd, crossd, 0)

        with scope("ugrad"):
            outer(s, acts, bpre, ugrad)

    loop(samples, gradient)
    pair_start(ugrad, pairu, 1)
    with scope("dnext"):
        cross_next(dgrad, paird, sendd, crossd, 0)
    with scope("ucross"):
        cross_start(ugrad, pairu, sendu, crossu, 1)
    with scope("unext"):
        cross_next(ugrad, pairu, sendu, crossu, 1)
    with scope("dfinish"):
        finish(dgrad, paird, sendd, crossd, 0, dg)
    with scope("ufinish"):
        finish(ugrad, pairu, sendu, crossu, 1, ug)

    for h in (0, 1):
        @pl.when(hop_of(h) < far)
        def _():
            loop(2 * chunks, lambda c: chunk_copy(h, c).wait_send())

        @pl.when(hop_of(h) > 0)
        def _():
            loop(chunks, lambda j: back_copy(h, j).wait_send())

    @pl.when(owner)
    def _():
        for s in range(samples):
            for offset in range(1, line):
                half_copy(s, offset).wait_send()

    for offset in range(1, group):
        cond_copy(offset).wait_send()
        for stage in range(2):
            mod_copy(stage, offset).wait_send()
    for offset in range(1, line):
        for stage in range(2):
            line_copy(stage, offset).wait_send()
    for w in range(4):
        for index in range(10):
            send(w, index).wait_send()


def fused_call(mesh, operands):
    samples = operands[0].shape[0]
    line = mesh.shape["col"]
    rows, hidden = operands[13].shape
    width = operands[11].shape[2]
    chips, group = 4, 8
    count = samples * SEQ
    chunks = samples * (D // BLOCK)
    f32, bf16 = jnp.float32, jnp.bfloat16
    vmem, dma = pltpu.VMEM, pltpu.SemaphoreType.DMA
    scratch = [
        vmem(operands[10].shape, bf16),
        vmem(operands[11].shape, bf16),
        vmem(operands[12].shape, bf16),
    ] + [vmem((D, hidden), bf16)] * 4 + [
        vmem((PATCH, count), f32),
        vmem((8, samples * TILE), f32),
        vmem((group, 8, rows), f32),
        vmem((group, 8, rows), f32),
        vmem((group, 6, 8, width), f32),
        vmem((group - 1, 6, 8, width), f32),
        vmem((line, 6, 8, width), f32),
        vmem((6, 8, D), f32),
        vmem((SEQ, D), bf16),
        vmem((count, D), bf16),
        vmem((count, hidden), bf16),
        vmem((count, hidden), bf16),
        vmem((count, hidden), f32),
        vmem((2, 2 * chunks, TILE, BLOCK), bf16),
        vmem((2, 2 * chunks, TILE, BLOCK), bf16),
        vmem((2 * chunks, TILE, BLOCK), f32),
        vmem((samples, TILE, TILE), f32),
        vmem((2, PATCH, samples * TILE), f32),
        vmem((PATCH, samples * TILE), f32),
        vmem((2, chunks, TILE, BLOCK), bf16),
        vmem((count, D), bf16),
        vmem((D, hidden), f32),
        vmem((D, hidden), f32),
        vmem((chips, rows, hidden), f32),
        vmem((chips, rows, hidden), f32),
        vmem((chips - 1, rows, hidden), bf16),
        vmem((chips - 1, rows, hidden), bf16),
        vmem((chips - 1, rows, hidden), bf16),
        vmem((chips - 1, rows, hidden), bf16),
        dma((7,)),
        dma((4, 10)), dma((4, 10)),
        dma((group - 1,)), dma((group - 1,)), dma((2, group - 1)), dma((2, group - 1)),
        dma((2, line - 1)), dma((2, line - 1)),
        dma((2, 2 * chunks)), dma((2, 2 * chunks)),
        dma((samples, line - 1)), dma((2, samples, line - 1)),
        dma((2, chunks)), dma((2, chunks)),
        dma((2, chips)), dma((2, chips)), dma((2, 6)), dma((2, 6)),
    ]

    def kernel(*refs):
        fused_kernel((mesh.shape["row"], line, samples, rows), *refs)

    specs = [pl.BlockSpec(memory_space=pltpu.SMEM)] * 3
    specs += [pl.BlockSpec(memory_space=pltpu.VMEM)] * 7
    specs += [pl.BlockSpec(memory_space=pl.ANY)] * 7
    return pl.pallas_call(
        kernel,
        out_shape=[pltpu.VMEM((rows, hidden), f32)] * 2,
        in_specs=specs,
        out_specs=[pl.BlockSpec(memory_space=pltpu.VMEM)] * 2,
        scratch_shapes=scratch,
        compiler_params=pltpu.CompilerParams(
            collective_id=0, has_side_effects=True, vmem_limit_bytes=65500000
        ),
    )(*operands)


def fused_body(mesh):
    def run(
        latents, labels, step_index, seeds, class_table,
        teacher_patch, teacher_mod, teacher_up, teacher_down, teacher_out,
        student_patch, student_mod, student_up, student_down, student_out,
    ):
        samples = latents.shape[0]
        lanes = latents.reshape(samples * SEQ, PATCH).T
        operands = (
            labels, step_index, seeds, lanes,
            jnp.asarray(position_tables()), jnp.asarray(feature_table()),
            teacher_patch, student_patch, teacher_out, student_out,
            class_table, teacher_mod.transpose(1, 0, 2), student_mod.transpose(1, 0, 2),
            teacher_up, teacher_down, student_up, student_down,
        )
        up_gradient, down_gradient = fused_call(mesh, operands)
        return up_gradient, down_gradient

    return run


def choose(mesh):
    sizes = dict(mesh.shape)
    fits = sizes["dp"] == 2 and sizes["row"] == 4 and sizes["col"] > 1
    return fused_body(mesh) if fits else body


def solution(mesh):
    placed = (
        P(("dp", "row"), None, None),
        P(("dp", "row")),
        P(("dp", "row")),
        P(("dp", "row")),
        P(),
        P(),
        P(("dp", "row"), None, "col"),
        P(("dp", "row"), "col"),
        P(("dp", "row"), "col"),
        P(),
        P(),
        P(("dp", "row"), None, "col"),
        P(("dp", "row"), "col"),
        P(("dp", "row"), "col"),
        P(),
    )
    return jax.shard_map(
        choose(mesh),
        mesh=mesh,
        in_specs=placed,
        out_specs=(P(("dp", "row"), "col"), P(("dp", "row"), "col")),
        check_vma=False,
    )
```
